16 devices in a mesh: dp: 16 (over z, y, x, core).
Axes of the slice: x: 2, y: 2, z: 2, core: 2. Of those that a mesh axis runs over, the one named last changes fastest.
Arguments:
- img_emb: bfloat16 [16384, 1152], P('dp')
- txt_emb: bfloat16 [16384, 1152], P('dp')
- log_temp: float32 [], replicated
- logit_bias: float32 [], replicated
Outputs:
- output 1: float32 [], replicated
- output 2: float32 [16384, 1152], P('dp')
- output 3: float32 [16384, 1152], P('dp')
- output 4: float32 [], replicated
- output 5: float32 [], replicated
All inputs are finite; a program needn't handle non-finite values.
Results may differ from the reference program's by a relative error of at most 0.001.
Values are sent between devices in bfloat16 or wider.
A program may use at most 1 GiB of HBM per device.

```python
import jax
import jax.numpy as jnp
from jax import lax

EMBED_DIM = 1152
ROWS_DEV = 1024
GROUP_SIZE = 16


def setup_inputs(seed: int = 0) -> dict:
    total_rows = ROWS_DEV * GROUP_SIZE
    num_groups = total_rows // 4
    unit_scale = EMBED_DIM ** -0.5
    rand_keys = jax.random.split(jax.random.key(seed), 10)
    shared_dir = jax.random.normal(rand_keys[0], (EMBED_DIM,), jnp.float32) * unit_scale
    centers = jax.random.normal(rand_keys[1], (num_groups, EMBED_DIM), jnp.float32) * unit_scale
    member = jax.random.randint(rand_keys[2], (total_rows,), 0, num_groups)
    own_part = jax.random.normal(rand_keys[3], (total_rows, EMBED_DIM), jnp.float32) * unit_scale
    img_noise = jax.random.normal(rand_keys[4], (total_rows, EMBED_DIM), jnp.float32) * unit_scale
    txt_noise = jax.random.normal(rand_keys[5], (total_rows, EMBED_DIM), jnp.float32) * unit_scale
    common = 0.47 * centers[member] + 0.28 * own_part
    img_scale = jax.random.uniform(rand_keys[6], (total_rows, 1), jnp.float32, minval=20.0, maxval=60.0)
    txt_scale = jax.random.uniform(rand_keys[7], (total_rows, 1), jnp.float32, minval=20.0, maxval=60.0)
    img_emb = (img_scale * (0.35 * shared_dir + common + 0.76 * img_noise)).astype(jnp.bfloat16)
    txt_emb = (txt_scale * (common - 0.35 * shared_dir + 0.76 * txt_noise)).astype(jnp.bfloat16)
    log_temp = jax.random.uniform(rand_keys[8], (), jnp.float32, minval=4.6, maxval=4.8)
    logit_bias = jax.random.uniform(rand_keys[9], (), jnp.float32, minval=-14.0, maxval=-10.0)
    return {"img_emb": img_emb, "txt_emb": txt_emb, "log_temp": log_temp, "logit_bias": logit_bias}


def normalize_rows(emb):
    emb32 = emb.astype(jnp.float32)
    inv_norm = lax.rsqrt(jnp.sum(emb32 * emb32, axis=-1, keepdims=True))
    return emb32 * inv_norm, inv_norm


def project_back(unit_rows, inv_norm, grad_dir):
    radial = jnp.sum(unit_rows * grad_dir, axis=-1, keepdims=True)
    return (grad_dir - unit_rows * radial) * inv_norm


def reference(img_emb, txt_emb, log_temp, logit_bias):
    total_rows = img_emb.shape[0]
    embed_width = img_emb.shape[1]
    block_rows = min(ROWS_DEV, 512)
    num_blocks = total_rows // block_rows
    img_unit, img_inv = normalize_rows(img_emb)
    txt_unit, txt_inv = normalize_rows(txt_emb)
    img_b = img_unit.astype(jnp.bfloat16)
    txt_b = txt_unit.astype(jnp.bfloat16)
    temp_scale = jnp.exp(log_temp)
    col_ids = jnp.arange(total_rows)

    def row_block(acc_state, block_in):
        x_blk, blk_idx = block_in
        loss_sum, weight_sum, weighted_sim, txt_grad = acc_state
        sim_vals = jnp.dot(x_blk, txt_b.T, preferred_element_type=jnp.float32)
        logits = temp_scale * sim_vals + logit_bias
        row_ids = blk_idx * block_rows + jnp.arange(block_rows)
        label_signs = jnp.where(row_ids[:, None] == col_ids[None, :], 1.0, -1.0)
        weights = -label_signs * jax.nn.sigmoid(-label_signs * logits)
        weights_b = weights.astype(jnp.bfloat16)
        new_state = (
            loss_sum + jnp.sum(jax.nn.softplus(-label_signs * logits)),
            weight_sum + jnp.sum(weights),
            weighted_sim + jnp.sum(weights * sim_vals),
            txt_grad + jnp.dot(weights_b.T, x_blk, preferred_element_type=jnp.float32),
        )
        return new_state, jnp.dot(weights_b, txt_b, preferred_element_type=jnp.float32)

    init_state = (
        jnp.zeros((), jnp.float32),
        jnp.zeros((), jnp.float32),
        jnp.zeros((), jnp.float32),
        jnp.zeros((total_rows, embed_width), jnp.float32),
    )
    blocks_in = (img_b.reshape(num_blocks, block_rows, embed_width), jnp.arange(num_blocks))
    final_state, img_parts = lax.scan(row_block, init_state, blocks_in)
    loss_sum, weight_sum, weighted_sim, txt_grad = final_state
    img_dir = temp_scale * img_parts.reshape(total_rows, embed_width)
    txt_dir = temp_scale * txt_grad
    loss_val = loss_sum / total_rows
    grad_img = project_back(img_unit, img_inv, img_dir)
    grad_txt = project_back(txt_unit, txt_inv, txt_dir)
    grad_log_temp = temp_scale * weighted_sim / total_rows
    grad_bias = weight_sum / total_rows
    return (loss_val, grad_img, grad_txt, grad_log_temp, grad_bias)
```

```python
import functools

import jax
import jax.numpy as jnp
from jax import lax
from jax.experimental import pallas as pl
from jax.experimental.pallas import tpu as pltpu
from jax.sharding import PartitionSpec as P

LOG2E = 1.4426950408889634
LN2 = 0.6931471805599453
MESH = pl.DeviceIdType.MESH
ROWS = 1024
WIDTH = 1152
PIECE = 512
HALVES = ROWS // PIECE
THIRD = WIDTH // 3
CORE, AX, AY, AZ = 1, 2, 4, 8
AXES = (AX, AY, AZ)

ORDER = (
    [(1, 0), (1, 1)]
    + [(m, 0) for m in (2, 4, 8, 3, 5, 9)]
    + [(m, 1) for m in (2, 4, 8, 3, 5, 9)]
    + [(m, 0) for m in (6, 12, 10, 7, 13, 11)]
    + [(m, 1) for m in (6, 12, 10, 7, 13, 11)]
    + [(14, 0), (15, 0), (14, 1), (15, 1)]
)
FORWARD = {
    2: [(AY, 384, 768, 0), (AZ, 384, 384, 0)],
    4: [(AZ, 0, 768, 0), (AX, 0, 384, 1)],
    8: [(AX, 0, 384, 1), (AX, 768, 384, 2), (AY, 768, 384, 1)],
    6: [(AZ, 384, 384, 0)],
    12: [(AX, 0, 384, 1)],
    10: [(AY, 768, 384, 2)],
}
PARTS = {1: [(0, WIDTH, 0)], 2: [(0, WIDTH, 0)], 4: [(0, WIDTH, 0)], 8: [(0, WIDTH, 0)]}
for _m, _sends in FORWARD.items():
    for _axis, _c0, _nc, _part in _sends:
        PARTS.setdefault(_m ^ _axis, []).append((_c0, _nc, _part))
for _m in (3, 5, 9, 7, 13, 11, 15):
    PARTS[_m] = [(0, WIDTH, 0)]


def normalize_rows(emb):
    emb32 = emb.astype(jnp.float32)
    inv_norm = lax.rsqrt(jnp.sum(emb32 * emb32, axis=-1, keepdims=True))
    return emb32 * inv_norm, inv_norm


def project_back(unit_rows, inv_norm, grad_dir):
    radial = jnp.sum(unit_rows * grad_dir, axis=-1, keepdims=True)
    return (grad_dir - unit_rows * radial) * inv_norm


def dot_t(a, b):
    return lax.dot_general(a, b, (((1,), (1,)), ((), ())), preferred_element_type=jnp.float32)


def dot_n(a, b):
    return lax.dot_general(a, b, (((1,), (0,)), ((), ())), preferred_element_type=jnp.float32)


def fold8(v):
    rows, cols = v.shape
    return jnp.sum(v.reshape(rows // 8, 8, cols), axis=0)


def text_weights(s, t2, b2, stats, row_off=None):
    rows, cols = s.shape
    step = 64
    out = []
    acc = [None, None, None]
    prod = None
    for r in range(0, rows, step):
        sc = s[r : r + step]
        logit = sc * t2 + b2
        small = jnp.exp2(-jnp.abs(logit))
        recip = 1.0 / (1.0 + small)
        other = small * recip
        pos = logit >= 0
        h = jnp.where(pos, recip, other)
        over = jnp.maximum(logit, 0.0)
        if row_off is not None:
            ri = lax.broadcasted_iota(jnp.int32, sc.shape, 0) + r
            ci = lax.broadcasted_iota(jnp.int32, sc.shape, 1) + row_off
            own = ri == ci
            h = jnp.where(own, -jnp.where(pos, other, recip), h)
            over = jnp.where(own, over - logit, over)
        sums = [fold8(over), fold8(h), fold8(h * sc)]
        acc = [b if a is None else a + b for a, b in zip(acc, sums)]
        q = small
        while q.shape[0] > 8:
            n = q.shape[0] // 2
            q = q[:n] + q[n:] + q[:n] * q[n:]
        if prod is None:
            prod = q
        elif (r // step) % 8 == 0:
            stats[3] += jnp.log1p(prod)
            prod = q
        else:
            prod = prod + q + prod * q
        out.append(h.astype(jnp.bfloat16))
    stats[3] += jnp.log1p(prod)
    for i in range(3):
        stats[i] += acc[i]
    return jnp.concatenate(out, axis=0)


def image_weights(s, t2, b2, row_off=None):
    logit = s * t2 + b2
    if row_off is None:
        return (1.0 / (1.0 + jnp.exp2(-logit))).astype(jnp.bfloat16)
    ri = lax.broadcasted_iota(jnp.int32, s.shape, 0)
    ci = lax.broadcasted_iota(jnp.int32, s.shape, 1) + row_off
    own = ri == ci
    h = 1.0 / (1.0 + jnp.exp2(jnp.where(own, logit, -logit)))
    return jnp.where(own, -h, h).astype(jnp.bfloat16)


def kernel(par, xb, yb, au, av, stats, land, xo, yo, bufs, own_sem, buf_sem, send_sem, recv_sem):
    me = lax.axis_index("dp")

    def peer(axis):
        return me + axis * (1 - 2 * lax.rem(me // axis, 2))

    barrier = pltpu.get_barrier_semaphore()
    for axis in (CORE,) + AXES:
        pl.semaphore_signal(barrier, inc=1, device_id=(peer(axis),), device_id_type=MESH)

    own_copies = [
        pltpu.make_async_copy(xb, xo, own_sem.at[0]),
        pltpu.make_async_copy(yb, yo, own_sem.at[1]),
    ]
    for c in own_copies:
        c.start()
    au[...] = jnp.zeros_like(au)
    av[...] = jnp.zeros_like(av)
    stats[...] = jnp.zeros_like(stats)
    pl.semaphore_wait(barrier, 4)

    started = []
    mine = (xb, yb)

    def rows(half):
        return pl.ds(half * PIECE, PIECE)

    def remote(src, owner, kind, half, c0, nc, part, axis, send_idx):
        return pltpu.make_async_remote_copy(
            src_ref=src,
            dst_ref=land.at[owner, kind, rows(half), pl.ds(c0, nc)],
            send_sem=send_sem.at[send_idx],
            recv_sem=recv_sem.at[owner, kind, half, part],
            device_id=(peer(axis),),
            device_id_type=MESH,
        )

    def send(*args):
        started.append(args[5])
        return remote(*args, len(started) - 1)

    for half in range(HALVES):
        for kind in (1, 0):
            for axis in (CORE,) + AXES:
                send(mine[kind].at[rows(half), :], axis, kind, half, 0, WIDTH, 0, axis).start()

    def local_copies(t, owner, half):
        slot = lax.rem(t, 2)
        return [
            pltpu.make_async_copy(land.at[owner, kind, rows(half), :], bufs.at[slot, kind], buf_sem.at[slot, kind])
            for kind in (0, 1)
        ]

    def arrive(p):
        owner, half = ORDER[p]
        for kind in (1, 0):
            for c0, nc, part in PARTS[owner]:
                view = land.at[owner, kind, rows(half), pl.ds(c0, nc)]
                remote(view, owner, kind, half, c0, nc, part, CORE, 0).wait_recv()
        for copy in local_copies(p, owner, half):
            copy.start()
        if owner % 2 == 0:
            for kind in (1, 0):
                whole = land.at[owner, kind, rows(half), :]
                send(whole, owner ^ CORE, kind, half, 0, WIDTH, 0, CORE).start()
                for axis, c0, nc, part in FORWARD.get(owner, []):
                    view = land.at[owner, kind, rows(half), pl.ds(c0, nc)]
                    send(view, owner ^ axis, kind, half, c0, nc, part, axis).start()

    t2 = par[0]
    b2 = par[1]

    def work(texts, images, row_off=None):
        sy = dot_t(xo[...], texts)
        sx = dot_t(yo[...], images)
        hy = text_weights(sy, t2, b2, stats, row_off)
        au[...] += dot_n(hy, texts)
        hx = image_weights(sx, t2, b2, row_off)
        av[...] += dot_n(hx, images)

    for c in own_copies:
        c.wait()

    def own_step(half, carry):
        off = pl.multiple_of(half * PIECE, PIECE)
        work(yo[pl.ds(off, PIECE), :], xo[pl.ds(off, PIECE), :], off)
        return carry

    lax.fori_loop(0, HALVES, own_step, 0)
    arrive(0)

    def at_step(t, lo, hi):
        if hi - lo == 1:
            arrive(lo + 1)
            return
        mid = (lo + hi) // 2

        @pl.when(t < mid)
        def _():
            at_step(t, lo, mid)

        @pl.when(t >= mid)
        def _():
            at_step(t, mid, hi)

    total = len(ORDER)

    def step(t, carry):
        for copy in local_copies(t, 1, 0):
            copy.wait()

        @pl.when(t < total - 1)
        def _():
            at_step(t, 0, total - 1)

        slot = lax.rem(t, 2)
        work(bufs[slot, 1], bufs[slot, 0])
        return carry

    lax.fori_loop(0, total, step, 0)
    for idx, cols in enumerate(started):
        view = land.at[1, 0, rows(0), pl.ds(0, cols)]
        remote(view, 1, 0, 0, 0, cols, 0, CORE, idx).wait_send()


N_SENDS = 2 * HALVES * (4 + 7 + sum(len(v) for v in FORWARD.values()))


def solution(mesh):
    group_size = mesh.shape["dp"]

    def local_fn(img_emb, txt_emb, log_temp, logit_bias):
        total_rows = ROWS * group_size
        img_unit, img_inv = normalize_rows(img_emb)
        txt_unit, txt_inv = normalize_rows(txt_emb)
        img_b = img_unit.astype(jnp.bfloat16)
        txt_b = txt_unit.astype(jnp.bfloat16)
        temp_scale = jnp.exp(log_temp)
        par = jnp.stack([temp_scale * LOG2E, logit_bias * LOG2E])
        hbm = pl.BlockSpec(memory_space=pl.ANY)
        vmem = pl.BlockSpec(memory_space=pltpu.VMEM)
        acc_shape = jax.ShapeDtypeStruct((ROWS, WIDTH), jnp.float32)
        au, av, stats, _ = pl.pallas_call(
            kernel,
            out_shape=(
                acc_shape,
                acc_shape,
                jax.ShapeDtypeStruct((4, 8, PIECE), jnp.float32),
                jax.ShapeDtypeStruct((16, 2, ROWS, WIDTH), jnp.bfloat16),
            ),
            in_specs=[pl.BlockSpec(memory_space=pltpu.SMEM), hbm, hbm],
            out_specs=(vmem, vmem, vmem, hbm),
            scratch_shapes=[
                pltpu.VMEM((ROWS, WIDTH), jnp.bfloat16),
                pltpu.VMEM((ROWS, WIDTH), jnp.bfloat16),
                pltpu.VMEM((2, 2, PIECE, WIDTH), jnp.bfloat16),
                pltpu.SemaphoreType.DMA((2,)),
                pltpu.SemaphoreType.DMA((2, 2)),
                pltpu.SemaphoreType.DMA((N_SENDS,)),
                pltpu.SemaphoreType.DMA((16, 2, HALVES, 3)),
            ],
            compiler_params=pltpu.CompilerParams(
                collective_id=0, has_side_effects=True, vmem_limit_bytes=60 * 2**20
            ),
        )(par, img_b, txt_b)
        sums = jnp.sum(stats, axis=(1, 2))
        local = jnp.stack([LN2 * sums[0] + sums[3], sums[1], sums[2]])
        total = lax.psum(local, "dp") / total_rows
        grad_img = project_back(img_unit, img_inv, temp_scale * au)
        grad_txt = project_back(txt_unit, txt_inv, temp_scale * av)
        return total[0], grad_img, grad_txt, temp_scale * total[2], total[1]

    return jax.shard_map(
        local_fn,
        mesh=mesh,
        in_specs=(P("dp", None), P("dp", None), P(), P()),
        out_specs=(P(), P("dp", None), P("dp", None), P(), P()),
        check_vma=False,
    )
```

```python
import jax
import jax.numpy as jnp
from jax import lax
from jax.experimental import pallas as pl
from jax.experimental.pallas import tpu as pltpu
from jax.sharding import PartitionSpec as P

LOG2E = 1.4426950408889634
LN2 = 0.6931471805599453
MESH = pl.DeviceIdType.MESH
ROWS = 1024
WIDTH = 1152
PIECE = 256
QUARTERS = ROWS // PIECE
CORE, AX, AY, AZ = 1, 2, 4, 8
AXES = (AX, AY, AZ)

FORWARD = {
    2: [(AY, 384, 768, 0), (AZ, 384, 384, 0)],
    4: [(AZ, 0, 768, 0), (AX, 0, 384, 1)],
    8: [(AX, 0, 384, 1), (AX, 768, 384, 2), (AY, 768, 384, 1)],
    6: [(AZ, 384, 384, 0)],
    12: [(AX, 0, 384, 1)],
    10: [(AY, 768, 384, 2)],
}
PARTS = {m: [(0, WIDTH, 0)] for m in (1, 2, 4, 8, 3, 5, 9, 7, 13, 11, 15)}
for _m, _sends in FORWARD.items():
    for _axis, _c0, _nc, _part in _sends:
        PARTS.setdefault(_m ^ _axis, []).append((_c0, _nc, _part))

_FAR = (6, 12, 10)
EVEN = [(m, q) for q in range(4) for m in AXES]
EVEN += [(m, q) for q in range(4) for m in _FAR]
EVEN += [(14, q) for q in range(4)]
_odd = [(m ^ CORE, q) for m, q in EVEN]
STEPS = [((1, 0), (1, 1)), (EVEN[0], (1, 2))]
STEPS += [(EVEN[k], _odd[k - 1]) for k in range(1, 27)]
STEPS += [(_odd[26], (1, 3)), (EVEN[27], _odd[27])]


def dot_t(a, b):
    return lax.dot_general(a, b, (((1,), (1,)), ((), ())), preferred_element_type=jnp.float32)


def dot_n(a, b):
    return lax.dot_general(a, b, (((1,), (0,)), ((), ())), preferred_element_type=jnp.float32)


def fold8(v):
    rows, cols = v.shape
    return jnp.sum(v.reshape(rows // 8, 8, cols), axis=0)


def text_weights(s, t2, b2, stats, row_off=None):
    rows, cols = s.shape
    step = 64
    out = []
    acc = [None, None, None]
    prod = None
    for r in range(0, rows, step):
        sc = s[r : r + step]
        logit = sc * t2 + b2
        small = jnp.exp2(-jnp.abs(logit))
        recip = 1.0 / (1.0 + small)
        other = small * recip
        pos = logit >= 0
        h = jnp.where(pos, recip, other)
        over = jnp.maximum(logit, 0.0)
        if row_off is not None:
            ri = lax.broadcasted_iota(jnp.int32, sc.shape, 0) + r
            ci = lax.broadcasted_iota(jnp.int32, sc.shape, 1) + row_off
            own = ri == ci
            h = jnp.where(own, -jnp.where(pos, other, recip), h)
            over = jnp.where(own, over - logit, over)
        sums = [fold8(over), fold8(h), fold8(h * sc)]
        acc = [b if a is None else a + b for a, b in zip(acc, sums)]
        q = small
        while q.shape[0] > 8:
            n = q.shape[0] // 2
            q = q[:n] + q[n:] + q[:n] * q[n:]
        if prod is None:
            prod = q
        elif (r // step) % 8 == 0:
            stats[3] += jnp.log1p(prod)
            prod = q
        else:
            prod = prod + q + prod * q
        out.append(h.astype(jnp.bfloat16))
    stats[3] += jnp.log1p(prod)
    for i in range(3):
        stats[i] += acc[i]
    return jnp.concatenate(out, axis=0)


def image_weights(s, t2, b2, row_off=None):
    logit = s * t2 + b2
    if row_off is None:
        return (1.0 / (1.0 + jnp.exp2(-logit))).astype(jnp.bfloat16)
    ri = lax.broadcasted_iota(jnp.int32, s.shape, 0)
    ci = lax.broadcasted_iota(jnp.int32, s.shape, 1) + row_off
    own = ri == ci
    h = 1.0 / (1.0 + jnp.exp2(jnp.where(own, logit, -logit)))
    return jnp.where(own, -h, h).astype(jnp.bfloat16)


def kernel(
    par, zx, zy, au, av, loss, gtemp, gbias, land, zxv, zyv, xo, yo, bufs, stats,
    own_sem, buf_sem, send_sem, recv_sem, stat_land, stat_send, stat_recv,
):
    me = lax.axis_index("dp")

    def peer(mask):
        at = me
        for bit in (1, 2, 4, 8):
            if mask & bit:
                at = at + bit * (1 - 2 * lax.rem(me // bit, 2))
        return at

    barrier = pltpu.get_barrier_semaphore()
    for mask in range(1, 16):
        pl.semaphore_signal(barrier, inc=1, device_id=(peer(mask),), device_id_type=MESH)

    arrays = ((zx, zxv, xo, au), (zy, zyv, yo, av))

    def rows(q):
        return pl.ds(q * PIECE, PIECE)

    def load(kind, q):
        src, dst = arrays[kind][:2]
        return pltpu.make_async_copy(src.at[rows(q), :], dst.at[rows(q), :], own_sem.at[kind, q])

    def unit_rows(z):
        z32 = z.astype(jnp.float32)
        inv = lax.rsqrt(jnp.sum(z32 * z32, axis=-1, keepdims=True))
        return z32 * inv, inv

    for q in range(QUARTERS):
        for kind in (1, 0):
            load(kind, q).start()
    for q in range(QUARTERS):
        for kind in (1, 0):
            load(kind, q).wait()
            _, raw, unit_b, _ = arrays[kind]
            unit_b[rows(q), :] = unit_rows(raw[rows(q), :])[0].astype(jnp.bfloat16)
    stats[...] = jnp.zeros_like(stats)
    au[...] = jnp.zeros_like(au)
    av[...] = jnp.zeros_like(av)
    pl.semaphore_wait(barrier, 15)

    started = []
    mine = (xo, yo)

    def remote(src, owner, kind, q, c0, nc, part, axis, send_idx):
        return pltpu.make_async_remote_copy(
            src_ref=src,
            dst_ref=land.at[owner, kind, rows(q), pl.ds(c0, nc)],
            send_sem=send_sem.at[send_idx],
            recv_sem=recv_sem.at[owner, kind, q, part],
            device_id=(peer(axis),),
            device_id_type=MESH,
        )

    def send(*args):
        started.append(args[5])
        return remote(*args, len(started) - 1)

    for q in range(QUARTERS):
        for kind in (1, 0):
            for axis in (CORE,) + AXES:
                send(mine[kind].at[rows(q), :], axis, kind, q, 0, WIDTH, 0, axis).start()

    def local_copy(t, owner, q, kind, chunk):
        slot = lax.rem(t, 2)
        return pltpu.make_async_copy(
            land.at[owner, kind, rows(q), :], bufs.at[slot, kind, rows(chunk), :], buf_sem.at[slot, kind, chunk]
        )

    def arrive(p):
        for chunk, (owner, q) in enumerate(STEPS[p]):
            for kind in (1, 0):
                for c0, nc, part in PARTS[owner]:
                    view = land.at[owner, kind, rows(q), pl.ds(c0, nc)]
                    remote(view, owner, kind, q, c0, nc, part, CORE, 0).wait_recv()
            if owner % 2 == 0:
                for kind in (1, 0):
                    whole = land.at[owner, kind, rows(q), :]
                    send(whole, owner ^ CORE, kind, q, 0, WIDTH, 0, CORE).start()
                    for axis, c0, nc, part in FORWARD.get(owner, []):
                        view = land.at[owner, kind, rows(q), pl.ds(c0, nc)]
                        send(view, owner ^ axis, kind, q, c0, nc, part, axis).start()
            for kind in (1, 0):
                local_copy(p, owner, q, kind, chunk).start()

    t2 = par[0]
    b2 = par[1]

    def work(texts, images, row_off=None):
        sy = dot_t(xo[...], texts)
        sx = dot_t(yo[...], images)
        hy = text_weights(sy, t2, b2, stats, row_off)
        au[...] += dot_n(hy, texts)
        hx = image_weights(sx, t2, b2, row_off)
        av[...] += dot_n(hx, images)

    def own_step(half, carry):
        off = pl.multiple_of(half * 2 * PIECE, 2 * PIECE)
        work(yo[pl.ds(off, 2 * PIECE), :], xo[pl.ds(off, 2 * PIECE), :], off)
        return carry

    lax.fori_loop(0, 2, own_step, 0)
    arrive(0)

    def at_step(t, lo, hi):
        if hi - lo == 1:
            arrive(lo + 1)
            return
        mid = (lo + hi) // 2

        @pl.when(t < mid)
        def _():
            at_step(t, lo, mid)

        @pl.when(t >= mid)
        def _():
            at_step(t, mid, hi)

    last = len(STEPS) - 1

    def step(t, carry):
        @pl.when(t < last - 1)
        def _():
            at_step(t, 0, last - 1)

        @pl.when(t == last)
        def _():
            arrive(last)

        for kind in (1, 0):
            for chunk in (0, 1):
                local_copy(t, 1, 0, kind, chunk).wait()
        slot = lax.rem(t, 2)
        work(bufs[slot, 1], bufs[slot, 0])
        return carry

    lax.fori_loop(0, last + 1, step, 0)

    acc = stats[...]
    stat_land[0] = acc[:, :, 0:128] + acc[:, :, 128:256] + acc[:, :, 256:384] + acc[:, :, 384:512]

    def stat_copy(mask):
        return pltpu.make_async_remote_copy(
            src_ref=stat_land.at[0],
            dst_ref=stat_land.at[mask],
            send_sem=stat_send.at[mask],
            recv_sem=stat_recv.at[mask],
            device_id=(peer(mask),),
            device_id_type=MESH,
        )

    for mask in range(15, 0, -1):
        stat_copy(mask).start()

    def project(i, carry):
        at = pl.ds(pl.multiple_of(i * 128, 128), 128)
        for _, raw, _, acc in arrays:
            unit, inv = unit_rows(raw[at, :])
            grad = par[2] * acc[at, :]
            radial = jnp.sum(unit * grad, axis=-1, keepdims=True)
            acc[at, :] = (grad - unit * radial) * inv
        return carry

    lax.fori_loop(0, ROWS // 128, project, 0)
    for idx, cols in enumerate(started):
        view = land.at[1, 0, rows(0), pl.ds(0, cols)]
        remote(view, 1, 0, 0, 0, cols, 0, CORE, idx).wait_send()
    for mask in range(1, 16):
        stat_copy(mask).wait()
    tree = [stat_land[m] for m in range(16)]
    while len(tree) > 1:
        tree = [tree[i] + tree[i + 1] for i in range(0, len(tree), 2)]
    total = tree[0]
    inv_rows = 1.0 / (ROWS * 16)
    loss[0] = (LN2 * jnp.sum(total[0]) + jnp.sum(total[3])) * inv_rows
    gbias[0] = jnp.sum(total[1]) * inv_rows
    gtemp[0] = par[2] * (jnp.sum(total[2]) * inv_rows)


N_SENDS = 2 * QUARTERS * (4 + 7 + sum(len(v) for v in FORWARD.values()))


def solution(mesh):
    def local_fn(img_emb, txt_emb, log_temp, logit_bias):
        temp_scale = jnp.exp(log_temp)
        par = jnp.stack([temp_scale * LOG2E, logit_bias * LOG2E, temp_scale])
        hbm = pl.BlockSpec(memory_space=pl.ANY)
        vmem = pl.BlockSpec(memory_space=pltpu.VMEM)
        smem = pl.BlockSpec(memory_space=pltpu.SMEM)
        acc_shape = jax.ShapeDtypeStruct((ROWS, WIDTH), jnp.float32)
        one = jax.ShapeDtypeStruct((1,), jnp.float32)
        whole = pltpu.VMEM((ROWS, WIDTH), jnp.bfloat16)
        gx, gy, loss, gtemp, gbias, _ = pl.pallas_call(
            kernel,
            out_shape=(
                acc_shape,
                acc_shape,
                one,
                one,
                one,
                jax.ShapeDtypeStruct((16, 2, ROWS, WIDTH), jnp.bfloat16),
            ),
            in_specs=[smem, hbm, hbm],
            out_specs=(vmem, vmem, smem, smem, smem, hbm),
            scratch_shapes=[
                whole,
                whole,
                whole,
                whole,
                pltpu.VMEM((2, 2, 2 * PIECE, WIDTH), jnp.bfloat16),
                pltpu.VMEM((4, 8, 2 * PIECE), jnp.float32),
                pltpu.SemaphoreType.DMA((2, QUARTERS)),
                pltpu.SemaphoreType.DMA((2, 2, 2)),
                pltpu.SemaphoreType.DMA((N_SENDS,)),
                pltpu.SemaphoreType.DMA((16, 2, QUARTERS, 3)),
                pltpu.VMEM((16, 4, 8, 128), jnp.float32),
                pltpu.SemaphoreType.DMA((16,)),
                pltpu.SemaphoreType.DMA((16,)),
            ],
            compiler_params=pltpu.CompilerParams(
                collective_id=0, has_side_effects=True, vmem_limit_bytes=62 * 2**20
            ),
        )(par, img_emb, txt_emb)
        return loss[0], gx, gy, gtemp[0], gbias[0]

    return jax.shard_map(
        local_fn,
        mesh=mesh,
        in_specs=(P("dp", None), P("dp", None), P(), P()),
        out_specs=(P(), P("dp", None), P("dp", None), P(), P()),
        check_vma=False,
    )
```

```python
import jax
import jax.numpy as jnp
from jax import lax
from jax.experimental import pallas as pl
from jax.experimental.pallas import tpu as pltpu
from jax.sharding import PartitionSpec as P

LOG2E = 1.4426950408889634
LN2 = 0.6931471805599453
MESH = pl.DeviceIdType.MESH
ROWS = 1024
WIDTH = 1152
PIECE = 256
LAG = 1
DIRECT = 20
QUARTERS = ROWS // PIECE
CORE, AX, AY, AZ = 1, 2, 4, 8
AXES = (AX, AY, AZ)

FORWARD = {
    2: [(AY, 384, 768, 0), (AZ, 384, 384, 0)],
    4: [(AZ, 0, 768, 0), (AX, 0, 384, 1)],
    8: [(AX, 0, 384, 1), (AX, 768, 384, 2), (AY, 768, 384, 1)],
    6: [(AZ, 384, 384, 0)],
    12: [(AX, 0, 384, 1)],
    10: [(AY, 768, 384, 2)],
}
PARTS = {m: [(0, WIDTH, 0)] for m in (1, 2, 4, 8, 3, 5, 9, 7, 13, 11, 15)}
for _m, _sends in FORWARD.items():
    for _axis, _c0, _nc, _part in _sends:
        PARTS.setdefault(_m ^ _axis, []).append((_c0, _nc, _part))

_FAR = (6, 12, 10)
EVEN = [(m, q) for q in range(4) for m in AXES]
EVEN += [(m, q) for q in range(4) for m in _FAR]
EVEN += [(14, q) for q in range(4)]
_odd = [(m ^ CORE, q) for m, q in EVEN]
STEPS = [((1, 0), (1, 1)), (EVEN[0], (1, 2))]
STEPS += [(EVEN[k], _odd[k - 1]) for k in range(1, 27)]
STEPS += [(_odd[26], (1, 3)), (EVEN[27], _odd[27])]


SPOT = {}
for _p in range(DIRECT, len(STEPS)):
    for _chunk, _piece in enumerate(STEPS[_p]):
        if _piece[0] != 1:
            SPOT[_piece] = (_p - DIRECT + 2, _chunk)


def is_late(p):
    if p >= DIRECT:
        return True
    return any(piece in EVEN and EVEN.index(piece) % 3 == 0 for piece in STEPS[p])


def dot_t(a, b):
    return lax.dot_general(a, b, (((1,), (1,)), ((), ())), preferred_element_type=jnp.float32)


def dot_n(a, b):
    return lax.dot_general(a, b, (((1,), (0,)), ((), ())), preferred_element_type=jnp.float32)


def fold8(v):
    rows, cols = v.shape
    return jnp.sum(v.reshape(rows // 8, 8, cols), axis=0)


def text_weights(s, t2, b2, stats, row_off=None):
    rows, cols = s.shape
    step = 64
    out = []
    acc = [None, None, None]
    prod = None
    for r in range(0, rows, step):
        sc = s[r : r + step]
        logit = sc * t2 + b2
        small = jnp.exp2(-jnp.abs(logit))
        recip = 1.0 / (1.0 + small)
        other = small * recip
        pos = logit >= 0
        h = jnp.where(pos, recip, other)
        over = jnp.maximum(logit, 0.0)
        if row_off is not None:
            ri = lax.broadcasted_iota(jnp.int32, sc.shape, 0) + r
            ci = lax.broadcasted_iota(jnp.int32, sc.shape, 1) + row_off
            own = ri == ci
            h = jnp.where(own, -jnp.where(pos, other, recip), h)
            over = jnp.where(own, over - logit, over)
        sums = [fold8(over), fold8(h), fold8(h * sc)]
        acc = [b if a is None else a + b for a, b in zip(acc, sums)]
        q = small
        while q.shape[0] > 8:
            n = q.shape[0] // 2
            q = q[:n] + q[n:] + q[:n] * q[n:]
        if prod is None:
            prod = q
        elif (r // step) % 8 == 0:
            stats[3] += jnp.log1p(prod)
            prod = q
        else:
            prod = prod + q + prod * q
        out.append(h.astype(jnp.bfloat16))
    stats[3] += jnp.log1p(prod)
    for i in range(3):
        stats[i] += acc[i]
    return jnp.concatenate(out, axis=0)


def image_weights(s, t2, b2, row_off=None):
    logit = s * t2 + b2
    if row_off is None:
        return (1.0 / (1.0 + jnp.exp2(-logit))).astype(jnp.bfloat16)
    ri = lax.broadcasted_iota(jnp.int32, s.shape, 0)
    ci = lax.broadcasted_iota(jnp.int32, s.shape, 1) + row_off
    own = ri == ci
    h = 1.0 / (1.0 + jnp.exp2(jnp.where(own, logit, -logit)))
    return jnp.where(own, -h, h).astype(jnp.bfloat16)


def unit_rows(z):
    z32 = z.astype(jnp.float32)
    inv = lax.rsqrt(jnp.sum(z32 * z32, axis=-1, keepdims=True))
    return z32 * inv, inv


def project_kernel(par, stats, zx, zy, au, av, gx, gy, loss, gtemp, gbias):
    for src, acc, dst in ((zx, au, gx), (zy, av, gy)):
        unit, inv = unit_rows(src[...])
        grad = par[2] * acc[...]
        radial = jnp.sum(unit * grad, axis=-1, keepdims=True)
        dst[...] = (grad - unit * radial) * inv

    @pl.when(pl.program_id(0) == 0)
    def _():
        inv_rows = 1.0 / (ROWS * 16)
        loss[0] = (LN2 * jnp.sum(stats[0]) + jnp.sum(stats[3])) * inv_rows
        gbias[0] = jnp.sum(stats[1]) * inv_rows
        gtemp[0] = par[2] * (jnp.sum(stats[2]) * inv_rows)


def kernel(
    par, zx, zy, out_u, out_v, total, land, xo, yo, au, av, bufs, stats,
    own_sem, buf_sem, out_sem, send_sem, recv_sem, stat_land, stat_send, stat_recv,
):
    me = lax.axis_index("dp")

    def peer(mask):
        at = me
        for bit in (1, 2, 4, 8):
            if mask & bit:
                at = at + bit * (1 - 2 * lax.rem(me // bit, 2))
        return at

    barrier = pltpu.get_barrier_semaphore()
    for mask in range(1, 16):
        pl.semaphore_signal(barrier, inc=1, device_id=(peer(mask),), device_id_type=MESH)

    arrays = ((zx, xo), (zy, yo))

    def rows(q):
        return pl.ds(q * PIECE, PIECE)

    def load(kind, q):
        src, dst = arrays[kind]
        return pltpu.make_async_copy(src.at[rows(q), :], dst.at[rows(q), :], own_sem.at[kind, q])

    for q in range(QUARTERS):
        for kind in (1, 0):
            load(kind, q).start()

    started = []
    mine = (xo, yo)

    def place(owner, kind, q, c0, nc):
        if (owner, q) in SPOT:
            slot, chunk = SPOT[owner, q]
            return bufs.at[slot, kind, rows(chunk), pl.ds(c0, nc)]
        return land.at[owner, kind, rows(q), pl.ds(c0, nc)]

    def remote(src, owner, kind, q, c0, nc, part, axis, send_idx):
        return pltpu.make_async_remote_copy(
            src_ref=src,
            dst_ref=place(owner, kind, q, c0, nc),
            send_sem=send_sem.at[send_idx],
            recv_sem=recv_sem.at[owner, kind, q, part],
            device_id=(peer(axis),),
            device_id_type=MESH,
        )

    def send(*args):
        started.append(args[5])
        return remote(*args, len(started) - 1)

    for q in range(QUARTERS):
        for kind in (1, 0):
            load(kind, q).wait()
            emb = arrays[kind][1]
            emb[rows(q), :] = unit_rows(emb[rows(q), :])[0].astype(jnp.bfloat16)
        if q == 0:
            pl.semaphore_wait(barrier, 15)
        for kind in (1, 0):
            for axis in (CORE,) + AXES:
                send(mine[kind].at[rows(q), :], axis, kind, q, 0, WIDTH, 0, axis).start()
    stats[...] = jnp.zeros_like(stats)
    au[...] = jnp.zeros_like(au)
    av[...] = jnp.zeros_like(av)

    def local_copy(p, owner, q, kind, chunk):
        return pltpu.make_async_copy(
            land.at[owner, kind, rows(q), :],
            bufs.at[slot_of(p), kind, rows(chunk), :],
            buf_sem.at[lax.rem(p, 2), kind, chunk],
        )

    def arrive(p, kind):
        for chunk, (owner, q) in enumerate(STEPS[p]):
            for c0, nc, part in PARTS[owner]:
                view = place(owner, kind, q, c0, nc)
                remote(view, owner, kind, q, c0, nc, part, CORE, 0).wait_recv()
            if owner % 2 == 0:
                whole = place(owner, kind, q, 0, WIDTH)
                send(whole, owner ^ CORE, kind, q, 0, WIDTH, 0, CORE).start()
                for axis, c0, nc, part in FORWARD.get(owner, []):
                    view = place(owner, kind, q, c0, nc)
                    send(view, owner ^ axis, kind, q, c0, nc, part, axis).start()
        for chunk, (owner, q) in enumerate(STEPS[p]):
            if (owner, q) not in SPOT:
                local_copy(p, owner, q, kind, chunk).start()
                if p >= DIRECT:
                    local_copy(p, owner, q, kind, chunk).wait()

    def slot_of(p):
        far = p // DIRECT
        return lax.rem(p, 2) * (1 - far) + (p - DIRECT + 2) * far

    def ready(p, kind):
        @pl.when(p < DIRECT)
        def _():
            for chunk in (0, 1):
                local_copy(p, 1, 0, kind, chunk).wait()

    last = len(STEPS) - 1
    t2 = par[0]
    b2 = par[1]

    def own_step(half, carry):
        off = pl.multiple_of(half * 2 * PIECE, 2 * PIECE)
        texts = yo[pl.ds(off, 2 * PIECE), :]
        images = xo[pl.ds(off, 2 * PIECE), :]
        sy = dot_t(xo[...], texts)
        sx = dot_t(yo[...], images)
        au[...] += dot_n(text_weights(sy, t2, b2, stats, off), texts)
        av[...] += dot_n(image_weights(sx, t2, b2, off), images)
        return carry

    def events(t, todo, lo, hi):
        if not any(todo.get(i) for i in range(lo, hi)):
            return
        if hi - lo == 1:
            for p, kind in todo[lo]:
                arrive(p, kind)
            return
        mid = (lo + hi) // 2

        @pl.when(t < mid)
        def _():
            events(t, todo, lo, mid)

        @pl.when(t >= mid)
        def _():
            events(t, todo, mid, hi)

    def phase(count, wanted, body):
        early = {t: [i for i in wanted(t) if not is_late(i[0])] for t in range(count)}
        late = {t: [i for i in wanted(t) if is_late(i[0])] for t in range(count)}

        def one(t, carry):
            events(t, early, 0, count)
            body(t)
            events(t, late, 0, count)
            return carry

        lax.fori_loop(0, count, one, 0)

    lax.fori_loop(0, 2, own_step, 0)
    arrive(0, 1)

    def text_step(t):
        ready(t, 1)
        texts = bufs[slot_of(t), 1]
        au[...] += dot_n(text_weights(dot_t(xo[...], texts), t2, b2, stats), texts)

    phase(LAG, lambda t: [(t + 1, 1)] + ([(0, 0)] if t == LAG - 1 else []), text_step)

    def pair_step(t):
        ready(t + LAG, 1)
        ready(t, 0)
        texts = bufs[slot_of(t + LAG), 1]
        images = bufs[slot_of(t), 0]
        sy = dot_t(xo[...], texts)
        sx = dot_t(yo[...], images)
        au[...] += dot_n(text_weights(sy, t2, b2, stats), texts)
        av[...] += dot_n(image_weights(sx, t2, b2), images)

    pairs = len(STEPS) - LAG
    phase(
        pairs,
        lambda t: ([(t + LAG + 1, 1)] if t + LAG < last else []) + ([(t + 1, 0)] if t + 1 < pairs else []),
        pair_step,
    )

    acc = stats[...]
    stat_land[0] = acc[:, :, 0:128] + acc[:, :, 128:256] + acc[:, :, 256:384] + acc[:, :, 384:512]

    def stat_copy(mask):
        return pltpu.make_async_remote_copy(
            src_ref=stat_land.at[0],
            dst_ref=stat_land.at[mask],
            send_sem=stat_send.at[mask],
            recv_sem=stat_recv.at[mask],
            device_id=(peer(mask),),
            device_id_type=MESH,
        )

    for mask in range(15, 0, -1):
        stat_copy(mask).start()
    flush_u = pltpu.make_async_copy(au, out_u, out_sem.at[0])
    flush_u.start()

    arrive(last, 0)
    images = bufs[slot_of(last), 0]
    av[...] += dot_n(image_weights(dot_t(yo[...], images), t2, b2), images)
    flush_v = pltpu.make_async_copy(av, out_v, out_sem.at[1])
    flush_v.start()
    for idx, cols in enumerate(started):
        view = land.at[1, 0, rows(0), pl.ds(0, cols)]
        remote(view, 1, 0, 0, 0, cols, 0, CORE, idx).wait_send()
    for mask in range(1, 16):
        stat_copy(mask).wait()
    tree = [stat_land[m] for m in range(16)]
    while len(tree) > 1:
        tree = [tree[i] + tree[i + 1] for i in range(0, len(tree), 2)]
    total[...] = tree[0]
    flush_u.wait()
    flush_v.wait()


N_SENDS = 2 * QUARTERS * (4 + 7 + sum(len(v) for v in FORWARD.values()))


def solution(mesh):
    def local_fn(img_emb, txt_emb, log_temp, logit_bias):
        temp_scale = jnp.exp(log_temp)
        par = jnp.stack([temp_scale * LOG2E, logit_bias * LOG2E, temp_scale])
        hbm = pl.BlockSpec(memory_space=pl.ANY)
        vmem = pl.BlockSpec(memory_space=pltpu.VMEM)
        smem = pl.BlockSpec(memory_space=pltpu.SMEM)
        block = pl.BlockSpec((256, WIDTH), lambda i: (i, 0))
        acc_shape = jax.ShapeDtypeStruct((ROWS, WIDTH), jnp.float32)
        one = jax.ShapeDtypeStruct((1,), jnp.float32)
        emb = pltpu.VMEM((ROWS, WIDTH), jnp.bfloat16)
        acc = pltpu.VMEM((ROWS, WIDTH), jnp.float32)
        au, av, stats, _ = pl.pallas_call(
            kernel,
            out_shape=(
                acc_shape,
                acc_shape,
                jax.ShapeDtypeStruct((4, 8, 128), jnp.float32),
                jax.ShapeDtypeStruct((16, 2, ROWS, WIDTH), jnp.bfloat16),
            ),
            in_specs=[smem, hbm, hbm],
            out_specs=(hbm, hbm, vmem, hbm),
            scratch_shapes=[
                emb,
                emb,
                acc,
                acc,
                pltpu.VMEM((2 + len(STEPS) - DIRECT, 2, 2 * PIECE, WIDTH), jnp.bfloat16),
                pltpu.VMEM((4, 8, 2 * PIECE), jnp.float32),
                pltpu.SemaphoreType.DMA((2, QUARTERS)),
                pltpu.SemaphoreType.DMA((2, 2, 2)),
                pltpu.SemaphoreType.DMA((2,)),
                pltpu.SemaphoreType.DMA((N_SENDS,)),
                pltpu.SemaphoreType.DMA((16, 2, QUARTERS, 3)),
                pltpu.VMEM((16, 4, 8, 128), jnp.float32),
                pltpu.SemaphoreType.DMA((16,)),
                pltpu.SemaphoreType.DMA((16,)),
            ],
            compiler_params=pltpu.CompilerParams(
                collective_id=0, has_side_effects=True, vmem_limit_bytes=62 * 2**20
            ),
        )(par, img_emb, txt_emb)
        gx, gy, loss, gtemp, gbias = pl.pallas_call(
            project_kernel,
            grid=(ROWS // 256,),
            out_shape=(acc_shape, acc_shape, one, one, one),
            in_specs=[smem, pl.BlockSpec((4, 8, 128), lambda i: (0, 0, 0)), block, block, block, block],
            out_specs=(block, block, smem, smem, smem),
        )(par, stats, img_emb, txt_emb, au, av)
        return loss[0], gx, gy, gtemp[0], gbias[0]

    return jax.shard_map(
        local_fn,
        mesh=mesh,
        in_specs=(P("dp", None), P("dp", None), P(), P()),
        out_specs=(P(), P("dp", None), P("dp", None), P(), P()),
        check_vma=False,
    )
```

```python
import jax
import jax.numpy as jnp
from jax import lax
from jax.experimental import pallas as pl
from jax.experimental.pallas import tpu as pltpu
from jax.sharding import PartitionSpec as P

LOG2E = 1.4426950408889634
LN2 = 0.6931471805599453
MESH = pl.DeviceIdType.MESH
ROWS = 1024
WIDTH = 1152
PIECE = 256
LAG = 1
DIRECT = 20
QUARTERS = ROWS // PIECE
CORE, AX, AY, AZ = 1, 2, 4, 8
AXES = (AX, AY, AZ)

FORWARD = {
    2: [(AY, 384, 768, 0), (AZ, 384, 384, 0)],
    4: [(AZ, 0, 768, 0), (AX, 0, 384, 1)],
    8: [(AX, 0, 384, 1), (AX, 768, 384, 2), (AY, 768, 384, 1)],
    6: [(AZ, 384, 384, 0)],
    12: [(AX, 0, 384, 1)],
    10: [(AY, 768, 384, 2)],
}
PARTS = {m: [(0, WIDTH, 0)] for m in (1, 2, 4, 8, 3, 5, 9, 7, 13, 11, 15)}
for _m, _sends in FORWARD.items():
    for _axis, _c0, _nc, _part in _sends:
        PARTS.setdefault(_m ^ _axis, []).append((_c0, _nc, _part))

_FAR = (6, 12, 10)
EVEN = [(m, q) for q in range(4) for m in AXES]
EVEN += [(m, q) for q in range(4) for m in _FAR]
EVEN += [(14, q) for q in range(4)]
_odd = [(m ^ CORE, q) for m, q in EVEN]
STEPS = [((1, 0), (1, 1)), ((1, 2), (1, 3)), (EVEN[0], EVEN[1]), (EVEN[2], _odd[0])]
STEPS += [(EVEN[k], _odd[k - 2]) for k in range(3, 28)]
STEPS += [(_odd[26], _odd[27])]

SPOT = {}
for _p in range(DIRECT, len(STEPS)):
    for _chunk, _piece in enumerate(STEPS[_p]):
        SPOT[_piece] = (_p - DIRECT + 2, _chunk)


def is_late(p):
    if p >= DIRECT:
        return True
    return any(piece in EVEN and EVEN.index(piece) % 3 == 0 for piece in STEPS[p])


def dot_t(a, b):
    return lax.dot_general(a, b, (((1,), (1,)), ((), ())), preferred_element_type=jnp.float32)


def dot_n(a, b):
    return lax.dot_general(a, b, (((1,), (0,)), ((), ())), preferred_element_type=jnp.float32)


def fold8(v):
    rows, cols = v.shape
    return jnp.sum(v.reshape(rows // 8, 8, cols), axis=0)


def text_weights(s, t2, b2, stats, row_off=None):
    rows, cols = s.shape
    step = 64
    out = []
    acc = [None, None, None]
    prod = None
    for r in range(0, rows, step):
        sc = s[r : r + step]
        logit = sc * t2 + b2
        small = jnp.exp2(-jnp.abs(logit))
        recip = 1.0 / (1.0 + small)
        other = small * recip
        pos = logit >= 0
        h = jnp.where(pos, recip, other)
        over = jnp.maximum(logit, 0.0)
        if row_off is not None:
            ri = lax.broadcasted_iota(jnp.int32, sc.shape, 0) + r
            ci = lax.broadcasted_iota(jnp.int32, sc.shape, 1) + row_off
            own = ri == ci
            h = jnp.where(own, -jnp.where(pos, other, recip), h)
            over = jnp.where(own, over - logit, over)
        sums = [fold8(over), fold8(h), fold8(h * sc)]
        acc = [b if a is None else a + b for a, b in zip(acc, sums)]
        q = small
        while q.shape[0] > 8:
            n = q.shape[0] // 2
            q = q[:n] + q[n:] + q[:n] * q[n:]
        if prod is None:
            prod = q
        elif (r // step) % 8 == 0:
            stats[3] += jnp.log1p(prod)
            prod = q
        else:
            prod = prod + q + prod * q
        out.append(h.astype(jnp.bfloat16))
    stats[3] += jnp.log1p(prod)
    for i in range(3):
        stats[i] += acc[i]
    return jnp.concatenate(out, axis=0)


def image_weights(s, t2, b2, row_off=None):
    logit = s * t2 + b2
    if row_off is None:
        return (1.0 / (1.0 + jnp.exp2(-logit))).astype(jnp.bfloat16)
    ri = lax.broadcasted_iota(jnp.int32, s.shape, 0)
    ci = lax.broadcasted_iota(jnp.int32, s.shape, 1) + row_off
    own = ri == ci
    h = 1.0 / (1.0 + jnp.exp2(jnp.where(own, logit, -logit)))
    return jnp.where(own, -h, h).astype(jnp.bfloat16)


def unit_rows(z):
    z32 = z.astype(jnp.float32)
    inv = lax.rsqrt(jnp.sum(z32 * z32, axis=-1, keepdims=True))
    return z32 * inv, inv


def project_kernel(stats, zx, zy, au, av, gx, gy, loss, gtemp, gbias):
    scale = stats[4][0:1, 0:1]
    for src, acc, dst in ((zx, au, gx), (zy, av, gy)):
        unit, inv = unit_rows(src[...])
        grad = scale * acc[...]
        radial = jnp.sum(unit * grad, axis=-1, keepdims=True)
        dst[...] = (grad - unit * radial) * inv

    @pl.when(pl.program_id(0) == 0)
    def _():
        inv_rows = 1.0 / (ROWS * 16)
        loss[0] = (LN2 * jnp.sum(stats[0]) + jnp.sum(stats[3])) * inv_rows
        gbias[0] = jnp.sum(stats[1]) * inv_rows
        gtemp[0] = jnp.max(stats[4]) * (jnp.sum(stats[2]) * inv_rows)


def kernel(
    log_temp, logit_bias, zx, zy, out_u, out_v, total, land, xo, yo, au, av, bufs, stats,
    own_sem, buf_sem, out_sem, send_sem, recv_sem, stat_land, stat_send, stat_recv,
):
    me = lax.axis_index("dp")

    def peer(mask):
        at = me
        for bit in (1, 2, 4, 8):
            if mask & bit:
                at = at + bit * (1 - 2 * lax.rem(me // bit, 2))
        return at

    barrier = pltpu.get_barrier_semaphore()
    for mask in range(1, 16):
        pl.semaphore_signal(barrier, inc=1, device_id=(peer(mask),), device_id_type=MESH)

    arrays = ((zx, xo), (zy, yo))

    def rows(q):
        return pl.ds(q * PIECE, PIECE)

    def load(kind, q):
        src, dst = arrays[kind]
        return pltpu.make_async_copy(src.at[rows(q), :], dst.at[rows(q), :], own_sem.at[kind, q])

    for q in range(QUARTERS):
        for kind in (1, 0):
            load(kind, q).start()

    started = []
    mine = (xo, yo)

    def place(owner, kind, q, c0, nc):
        if (owner, q) in SPOT:
            slot, chunk = SPOT[owner, q]
            return bufs.at[slot, kind, rows(chunk), pl.ds(c0, nc)]
        return land.at[owner, kind, rows(q), pl.ds(c0, nc)]

    def remote(src, owner, kind, q, c0, nc, part, axis, send_idx):
        return pltpu.make_async_remote_copy(
            src_ref=src,
            dst_ref=place(owner, kind, q, c0, nc),
            send_sem=send_sem.at[send_idx],
            recv_sem=recv_sem.at[owner, kind, q, part],
            device_id=(peer(axis),),
            device_id_type=MESH,
        )

    def send(*args):
        started.append(args[5])
        return remote(*args, len(started) - 1)

    for q in range(QUARTERS):
        for kind in (1, 0):
            load(kind, q).wait()
            emb = arrays[kind][1]
            emb[rows(q), :] = unit_rows(emb[rows(q), :])[0].astype(jnp.bfloat16)
        if q == 0:
            pl.semaphore_wait(barrier, 15)
        for kind in (1, 0):
            for axis in (CORE,) + AXES:
                send(mine[kind].at[rows(q), :], axis, kind, q, 0, WIDTH, 0, axis).start()
    stats[...] = jnp.zeros_like(stats)
    au[...] = jnp.zeros_like(au)
    av[...] = jnp.zeros_like(av)

    def local_copy(p, owner, q, kind, chunk):
        return pltpu.make_async_copy(
            land.at[owner, kind, rows(q), :],
            bufs.at[slot_of(p), kind, rows(chunk), :],
            buf_sem.at[lax.rem(p, 2), kind, chunk],
        )

    def arrive(p, kind):
        for chunk, (owner, q) in enumerate(STEPS[p]):
            for c0, nc, part in PARTS[owner]:
                view = place(owner, kind, q, c0, nc)
                remote(view, owner, kind, q, c0, nc, part, CORE, 0).wait_recv()
            if owner % 2 == 0:
                whole = place(owner, kind, q, 0, WIDTH)
                send(whole, owner ^ CORE, kind, q, 0, WIDTH, 0, CORE).start()
                for axis, c0, nc, part in FORWARD.get(owner, []):
                    view = place(owner, kind, q, c0, nc)
                    send(view, owner ^ axis, kind, q, c0, nc, part, axis).start()
        for chunk, (owner, q) in enumerate(STEPS[p]):
            if p < DIRECT:
                local_copy(p, owner, q, kind, chunk).start()

    def slot_of(p):
        far = p // DIRECT
        return lax.rem(p, 2) * (1 - far) + (p - DIRECT + 2) * far

    def ready(p, kind):
        @pl.when(p < DIRECT)
        def _():
            for chunk in (0, 1):
                local_copy(p, 1, 0, kind, chunk).wait()

    last = len(STEPS) - 1
    scale = jnp.exp(jnp.full((8, 128), log_temp[0], jnp.float32))
    t2 = jnp.max(scale) * LOG2E
    b2 = logit_bias[0] * LOG2E

    def own_step(half, carry):
        off = pl.multiple_of(half * 2 * PIECE, 2 * PIECE)
        texts = yo[pl.ds(off, 2 * PIECE), :]
        images = xo[pl.ds(off, 2 * PIECE), :]
        sy = dot_t(xo[...], texts)
        sx = dot_t(yo[...], images)
        au[...] += dot_n(text_weights(sy, t2, b2, stats, off), texts)
        av[...] += dot_n(image_weights(sx, t2, b2, off), images)
        return carry

    def events(t, todo, lo, hi):
        if not any(todo.get(i) for i in range(lo, hi)):
            return
        if hi - lo == 1:
            for p, kind in todo[lo]:
                arrive(p, kind)
            return
        mid = (lo + hi) // 2

        @pl.when(t < mid)
        def _():
            events(t, todo, lo, mid)

        @pl.when(t >= mid)
        def _():
            events(t, todo, mid, hi)

    def phase(count, wanted, body):
        early = {t: [i for i in wanted(t) if not is_late(i[0])] for t in range(count)}
        late = {t: [i for i in wanted(t) if is_late(i[0])] for t in range(count)}

        def one(t, carry):
            events(t, early, 0, count)
            body(t)
            events(t, late, 0, count)
            return carry

        lax.fori_loop(0, count, one, 0)

    lax.fori_loop(0, 2, own_step, 0)
    arrive(0, 1)

    def text_step(t):
        ready(t, 1)
        texts = bufs[slot_of(t), 1]
        au[...] += dot_n(text_weights(dot_t(xo[...], texts), t2, b2, stats), texts)

    phase(LAG, lambda t: [(t + 1, 1)] + ([(0, 0)] if t == LAG - 1 else []), text_step)

    def pair_step(t):
        ready(t + LAG, 1)
        ready(t, 0)
        texts = bufs[slot_of(t + LAG), 1]
        images = bufs[slot_of(t), 0]
        sy = dot_t(xo[...], texts)
        sx = dot_t(yo[...], images)
        au[...] += dot_n(text_weights(sy, t2, b2, stats), texts)
        av[...] += dot_n(image_weights(sx, t2, b2), images)

    pairs = len(STEPS) - LAG
    phase(
        pairs,
        lambda t: ([(t + LAG + 1, 1)] if t + LAG < last else []) + ([(t + 1, 0)] if t + 1 < pairs else []),
        pair_step,
    )

    acc = stats[...]
    stat_land[0] = acc[:, :, 0:128] + acc[:, :, 128:256] + acc[:, :, 256:384] + acc[:, :, 384:512]

    def stat_copy(mask):
        return pltpu.make_async_remote_copy(
            src_ref=stat_land.at[0],
            dst_ref=stat_land.at[mask],
            send_sem=stat_send.at[mask],
            recv_sem=stat_recv.at[mask],
            device_id=(peer(mask),),
            device_id_type=MESH,
        )

    for mask in range(15, 0, -1):
        stat_copy(mask).start()
    flush_u = pltpu.make_async_copy(au, out_u, out_sem.at[0])
    flush_u.start()

    arrive(last, 0)
    images = bufs[slot_of(last), 0]
    av[...] += dot_n(image_weights(dot_t(yo[...], images), t2, b2), images)
    flush_v = pltpu.make_async_copy(av, out_v, out_sem.at[1])
    flush_v.start()
    for idx, cols in enumerate(started):
        view = land.at[1, 0, rows(0), pl.ds(0, cols)]
        remote(view, 1, 0, 0, 0, cols, 0, CORE, idx).wait_send()
    for mask in range(1, 16):
        stat_copy(mask).wait()
    tree = [stat_land[m] for m in range(16)]
    while len(tree) > 1:
        tree = [tree[i] + tree[i + 1] for i in range(0, len(tree), 2)]
    total[0:4] = tree[0]
    total[4] = scale
    flush_u.wait()
    flush_v.wait()


N_SENDS = 2 * QUARTERS * (4 + 7 + sum(len(v) for v in FORWARD.values()))


def solution(mesh):
    def local_fn(img_emb, txt_emb, log_temp, logit_bias):
        hbm = pl.BlockSpec(memory_space=pl.ANY)
        vmem = pl.BlockSpec(memory_space=pltpu.VMEM)
        smem = pl.BlockSpec(memory_space=pltpu.SMEM)
        block = pl.BlockSpec((512, WIDTH), lambda i: (i, 0))
        acc_shape = jax.ShapeDtypeStruct((ROWS, WIDTH), jnp.float32)
        one = jax.ShapeDtypeStruct((1,), jnp.float32)
        emb = pltpu.VMEM((ROWS, WIDTH), jnp.bfloat16)
        acc = pltpu.VMEM((ROWS, WIDTH), jnp.float32)
        au, av, stats, _ = pl.pallas_call(
            kernel,
            out_shape=(
                acc_shape,
                acc_shape,
                jax.ShapeDtypeStruct((5, 8, 128), jnp.float32),
                jax.ShapeDtypeStruct((16, 2, ROWS, WIDTH), jnp.bfloat16),
            ),
            in_specs=[smem, smem, hbm, hbm],
            out_specs=(hbm, hbm, vmem, hbm),
            scratch_shapes=[
                emb,
                emb,
                acc,
                acc,
                pltpu.VMEM((2 + len(STEPS) - DIRECT, 2, 2 * PIECE, WIDTH), jnp.bfloat16),
                pltpu.VMEM((4, 8, 2 * PIECE), jnp.float32),
                pltpu.SemaphoreType.DMA((2, QUARTERS)),
                pltpu.SemaphoreType.DMA((2, 2, 2)),
                pltpu.SemaphoreType.DMA((2,)),
                pltpu.SemaphoreType.DMA((N_SENDS,)),
                pltpu.SemaphoreType.DMA((16, 2, QUARTERS, 3)),
                pltpu.VMEM((16, 4, 8, 128), jnp.float32),
                pltpu.SemaphoreType.DMA((16,)),
                pltpu.SemaphoreType.DMA((16,)),
            ],
            compiler_params=pltpu.CompilerParams(
                collective_id=0, has_side_effects=True, vmem_limit_bytes=62 * 2**20
            ),
        )(log_temp.reshape(1), logit_bias.reshape(1), img_emb, txt_emb)
        gx, gy, loss, gtemp, gbias = pl.pallas_call(
            project_kernel,
            grid=(ROWS // 512,),
            out_shape=(acc_shape, acc_shape, one, one, one),
            in_specs=[pl.BlockSpec((5, 8, 128), lambda i: (0, 0, 0)), block, block, block, block],
            out_specs=(block, block, smem, smem, smem),
        )(stats, img_emb, txt_emb, au, av)
        return loss[0], gx, gy, gtemp[0], gbias[0]

    return jax.shard_map(
        local_fn,
        mesh=mesh,
        in_specs=(P("dp", None), P("dp", None), P(), P()),
        out_specs=(P(), P("dp", None), P("dp", None), P(), P()),
        check_vma=False,
    )
```

```python
import jax
import jax.numpy as jnp
from jax import lax
from jax.experimental import pallas as pl
from jax.experimental.pallas import tpu as pltpu
from jax.sharding import PartitionSpec as P

LOG2E = 1.4426950408889634
LN2 = 0.6931471805599453
MESH = pl.DeviceIdType.MESH
ROWS = 1024
WIDTH = 1152
PIECE = 256
LAG = 1
DIRECT = 20
QUARTERS = ROWS // PIECE
CORE, AX, AY, AZ = 1, 2, 4, 8
AXES = (AX, AY, AZ)

FORWARD = {
    2: [(AY, 384, 768, 0), (AZ, 384, 384, 0)],
    4: [(AZ, 0, 768, 0), (AX, 0, 384, 1)],
    8: [(AX, 0, 384, 1), (AX, 768, 384, 2), (AY, 768, 384, 1)],
    6: [(AZ, 384, 384, 0)],
    12: [(AX, 0, 384, 1)],
    10: [(AY, 768, 384, 2)],
}
PARTS = {m: [(0, WIDTH, 0)] for m in (1, 2, 4, 8, 3, 5, 9, 7, 13, 11, 15)}
for _m, _sends in FORWARD.items():
    for _axis, _c0, _nc, _part in _sends:
        PARTS.setdefault(_m ^ _axis, []).append((_c0, _nc, _part))

_FAR = (6, 12, 10)
EVEN = [(m, q) for q in range(4) for m in AXES]
EVEN += [(m, q) for q in range(4) for m in _FAR]
EVEN += [(14, q) for q in range(4)]
_odd = [(m ^ CORE, q) for m, q in EVEN]
STEPS = [((1, 0), (1, 1)), ((1, 2), (1, 3)), (EVEN[0], EVEN[1]), (EVEN[2], _odd[0])]
STEPS += [(EVEN[k], _odd[k - 2]) for k in range(3, 28)]
STEPS += [(_odd[26], _odd[27])]

SPOT = {}
for _p in range(DIRECT, len(STEPS)):
    for _chunk, _piece in enumerate(STEPS[_p]):
        SPOT[_piece] = (_p - DIRECT + 2, _chunk)


def is_late(p):
    if p >= DIRECT:
        return True
    return any(piece in EVEN and EVEN.index(piece) % 3 == 0 for piece in STEPS[p])


def dot_t(a, b):
    return lax.dot_general(a, b, (((1,), (1,)), ((), ())), preferred_element_type=jnp.float32)


def dot_n(a, b):
    return lax.dot_general(a, b, (((1,), (0,)), ((), ())), preferred_element_type=jnp.float32)


def fold8(v):
    rows, cols = v.shape
    return jnp.sum(v.reshape(rows // 8, 8, cols), axis=0)


def text_weights(s, t2, b2, stats, row_off=None):
    rows, cols = s.shape
    step = 64
    out = []
    acc = [None, None, None]
    prod = None
    for r in range(0, rows, step):
        sc = s[r : r + step]
        logit = sc * t2 + b2
        small = jnp.exp2(-jnp.abs(logit))
        recip = 1.0 / (1.0 + small)
        other = small * recip
        pos = logit >= 0
        h = jnp.where(pos, recip, other)
        over = jnp.maximum(logit, 0.0)
        if row_off is not None:
            ri = lax.broadcasted_iota(jnp.int32, sc.shape, 0) + r
            ci = lax.broadcasted_iota(jnp.int32, sc.shape, 1) + row_off
            own = ri == ci
            h = jnp.where(own, -jnp.where(pos, other, recip), h)
            over = jnp.where(own, over - logit, over)
        sums = [fold8(over), fold8(h), fold8(h * sc)]
        acc = [b if a is None else a + b for a, b in zip(acc, sums)]
        q = small
        while q.shape[0] > 8:
            n = q.shape[0] // 2
            q = q[:n] + q[n:] + q[:n] * q[n:]
        if prod is None:
            prod = q
        elif (r // step) % 8 == 0:
            stats[3] += jnp.log1p(prod)
            prod = q
        else:
            prod = prod + q + prod * q
        out.append(h.astype(jnp.bfloat16))
    stats[3] += jnp.log1p(prod)
    for i in range(3):
        stats[i] += acc[i]
    return jnp.concatenate(out, axis=0)


def image_weights(s, t2, b2, row_off=None):
    logit = s * t2 + b2
    if row_off is None:
        return (1.0 / (1.0 + jnp.exp2(-logit))).astype(jnp.bfloat16)
    ri = lax.broadcasted_iota(jnp.int32, s.shape, 0)
    ci = lax.broadcasted_iota(jnp.int32, s.shape, 1) + row_off
    own = ri == ci
    h = 1.0 / (1.0 + jnp.exp2(jnp.where(own, logit, -logit)))
    return jnp.where(own, -h, h).astype(jnp.bfloat16)


def unit_rows(z):
    z32 = z.astype(jnp.float32)
    inv = lax.rsqrt(jnp.sum(z32 * z32, axis=-1, keepdims=True))
    return z32 * inv, inv


def project_kernel(stats, zx, zy, au, av, gx, gy, loss, gtemp, gbias):
    scale = stats[4][0:1, 0:1]
    for src, acc, dst in ((zx, au, gx), (zy, av, gy)):
        unit, inv = unit_rows(src[...])
        grad = scale * acc[...]
        radial = jnp.sum(unit * grad, axis=-1, keepdims=True)
        dst[...] = (grad - unit * radial) * inv

    @pl.when(pl.program_id(0) == 0)
    def _():
        inv_rows = 1.0 / (ROWS * 16)
        loss[0] = (LN2 * jnp.sum(stats[0]) + jnp.sum(stats[3])) * inv_rows
        gbias[0] = jnp.sum(stats[1]) * inv_rows
        gtemp[0] = jnp.max(stats[4]) * (jnp.sum(stats[2]) * inv_rows)


def kernel(
    log_temp, logit_bias, zx, zy, out_u, out_v, total, land, xo, yo, au, av, bufs, stats,
    own_sem, buf_sem, out_sem, send_sem, recv_sem, stat_land, stat_send, stat_recv,
):
    me = lax.axis_index("dp")

    def peer(mask):
        at = me
        for bit in (1, 2, 4, 8):
            if mask & bit:
                at = at + bit * (1 - 2 * lax.rem(me // bit, 2))
        return at

    barrier = pltpu.get_barrier_semaphore()
    for mask in range(1, 16):
        pl.semaphore_signal(barrier, inc=1, device_id=(peer(mask),), device_id_type=MESH)

    arrays = ((zx, xo), (zy, yo))

    def rows(q):
        return pl.ds(q * PIECE, PIECE)

    def load(kind, q):
        src, dst = arrays[kind]
        return pltpu.make_async_copy(src.at[rows(q), :], dst.at[rows(q), :], own_sem.at[kind, q])

    for q in range(QUARTERS):
        for kind in (1, 0):
            load(kind, q).start()

    started = []
    mine = (xo, yo)

    def place(owner, kind, q, c0, nc):
        if (owner, q) in SPOT:
            slot, chunk = SPOT[owner, q]
            return bufs.at[slot, kind, rows(chunk), pl.ds(c0, nc)]
        return land.at[owner, kind, rows(q), pl.ds(c0, nc)]

    def remote(src, owner, kind, q, c0, nc, part, axis, send_idx):
        return pltpu.make_async_remote_copy(
            src_ref=src,
            dst_ref=place(owner, kind, q, c0, nc),
            send_sem=send_sem.at[send_idx],
            recv_sem=recv_sem.at[owner, kind, q, part],
            device_id=(peer(axis),),
            device_id_type=MESH,
        )

    def send(*args):
        started.append(args[5])
        return remote(*args, len(started) - 1)

    for q in range(QUARTERS):
        for kind in (1, 0):
            load(kind, q).wait()
            emb = arrays[kind][1]
            emb[rows(q), :] = unit_rows(emb[rows(q), :])[0].astype(jnp.bfloat16)
            if q == 0 and kind == 1:
                pl.semaphore_wait(barrier, 15)
            for axis in AXES + (CORE,):
                send(mine[kind].at[rows(q), :], axis, kind, q, 0, WIDTH, 0, axis).start()
    stats[...] = jnp.zeros_like(stats)
    au[...] = jnp.zeros_like(au)
    av[...] = jnp.zeros_like(av)

    def local_copy(p, owner, q, kind, chunk):
        return pltpu.make_async_copy(
            land.at[owner, kind, rows(q), :],
            bufs.at[slot_of(p), kind, rows(chunk), :],
            buf_sem.at[lax.rem(p, 2), kind, chunk],
        )

    def arrive(p, kind):
        for chunk, (owner, q) in enumerate(STEPS[p]):
            for c0, nc, part in PARTS[owner]:
                view = place(owner, kind, q, c0, nc)
                remote(view, owner, kind, q, c0, nc, part, CORE, 0).wait_recv()
            if owner % 2 == 0:
                whole = place(owner, kind, q, 0, WIDTH)
                send(whole, owner ^ CORE, kind, q, 0, WIDTH, 0, CORE).start()
                for axis, c0, nc, part in FORWARD.get(owner, []):
                    view = place(owner, kind, q, c0, nc)
                    send(view, owner ^ axis, kind, q, c0, nc, part, axis).start()
        for chunk, (owner, q) in enumerate(STEPS[p]):
            if p < DIRECT:
                local_copy(p, owner, q, kind, chunk).start()

    def slot_of(p):
        far = p // DIRECT
        return lax.rem(p, 2) * (1 - far) + (p - DIRECT + 2) * far

    def ready(p, kind):
        @pl.when(p < DIRECT)
        def _():
            for chunk in (0, 1):
                local_copy(p, 1, 0, kind, chunk).wait()

    last = len(STEPS) - 1
    scale = jnp.exp(jnp.full((8, 128), log_temp[0], jnp.float32))
    t2 = jnp.max(scale) * LOG2E
    b2 = logit_bias[0] * LOG2E

    def own_step(half, carry):
        off = pl.multiple_of(half * 2 * PIECE, 2 * PIECE)
        texts = yo[pl.ds(off, 2 * PIECE), :]
        images = xo[pl.ds(off, 2 * PIECE), :]
        sy = dot_t(xo[...], texts)
        sx = dot_t(yo[...], images)
        au[...] += dot_n(text_weights(sy, t2, b2, stats, off), texts)
        av[...] += dot_n(image_weights(sx, t2, b2, off), images)
        return carry

    def events(t, todo, lo, hi):
        if not any(todo.get(i) for i in range(lo, hi)):
            return
        if hi - lo == 1:
            for p, kind in todo[lo]:
                arrive(p, kind)
            return
        mid = (lo + hi) // 2

        @pl.when(t < mid)
        def _():
            events(t, todo, lo, mid)

        @pl.when(t >= mid)
        def _():
            events(t, todo, mid, hi)

    def phase(count, wanted, body):
        early = {t: [i for i in wanted(t) if not is_late(i[0])] for t in range(count)}
        late = {t: [i for i in wanted(t) if is_late(i[0])] for t in range(count)}

        def one(t, carry):
            events(t, early, 0, count)
            body(t)
            events(t, late, 0, count)
            return carry

        lax.fori_loop(0, count, one, 0)

    lax.fori_loop(0, 2, own_step, 0)
    arrive(0, 1)

    def text_step(t):
        ready(t, 1)
        texts = bufs[slot_of(t), 1]
        au[...] += dot_n(text_weights(dot_t(xo[...], texts), t2, b2, stats), texts)

    phase(LAG, lambda t: [(t + 1, 1)] + ([(0, 0)] if t == LAG - 1 else []), text_step)

    def pair_step(t):
        ready(t + LAG, 1)
        ready(t, 0)
        texts = bufs[slot_of(t + LAG), 1]
        images = bufs[slot_of(t), 0]
        sy = dot_t(xo[...], texts)
        sx = dot_t(yo[...], images)
        au[...] += dot_n(text_weights(sy, t2, b2, stats), texts)
        av[...] += dot_n(image_weights(sx, t2, b2), images)

    pairs = len(STEPS) - LAG
    phase(
        pairs,
        lambda t: ([(t + LAG + 1, 1)] if t + LAG < last else []) + ([(t + 1, 0)] if t + 1 < pairs else []),
        pair_step,
    )

    acc = stats[...]
    stat_land[0] = acc[:, :, 0:128] + acc[:, :, 128:256] + acc[:, :, 256:384] + acc[:, :, 384:512]

    def stat_copy(mask):
        return pltpu.make_async_remote_copy(
            src_ref=stat_land.at[0],
            dst_ref=stat_land.at[mask],
            send_sem=stat_send.at[mask],
            recv_sem=stat_recv.at[mask],
            device_id=(peer(mask),),
            device_id_type=MESH,
        )

    for mask in range(15, 0, -1):
        stat_copy(mask).start()
    flush_u = pltpu.make_async_copy(au, out_u, out_sem.at[0])
    flush_u.start()

    arrive(last, 0)
    images = bufs[slot_of(last), 0]
    av[...] += dot_n(image_weights(dot_t(yo[...], images), t2, b2), images)
    flush_v = pltpu.make_async_copy(av, out_v, out_sem.at[1])
    flush_v.start()
    for idx, cols in enumerate(started):
        view = land.at[1, 0, rows(0), pl.ds(0, cols)]
        remote(view, 1, 0, 0, 0, cols, 0, CORE, idx).wait_send()
    for mask in range(1, 16):
        stat_copy(mask).wait()
    tree = [stat_land[m] for m in range(16)]
    while len(tree) > 1:
        tree = [tree[i] + tree[i + 1] for i in range(0, len(tree), 2)]
    total[0:4] = tree[0]
    total[4] = scale
    flush_u.wait()
    flush_v.wait()


N_SENDS = 2 * QUARTERS * (4 + 7 + sum(len(v) for v in FORWARD.values()))


def solution(mesh):
    def local_fn(img_emb, txt_emb, log_temp, logit_bias):
        hbm = pl.BlockSpec(memory_space=pl.ANY)
        vmem = pl.BlockSpec(memory_space=pltpu.VMEM)
        smem = pl.BlockSpec(memory_space=pltpu.SMEM)
        block = pl.BlockSpec((512, WIDTH), lambda i: (i, 0))
        acc_shape = jax.ShapeDtypeStruct((ROWS, WIDTH), jnp.float32)
        one = jax.ShapeDtypeStruct((1,), jnp.float32)
        emb = pltpu.VMEM((ROWS, WIDTH), jnp.bfloat16)
        acc = pltpu.VMEM((ROWS, WIDTH), jnp.float32)
        au, av, stats, _ = pl.pallas_call(
            kernel,
            out_shape=(
                acc_shape,
                acc_shape,
                jax.ShapeDtypeStruct((5, 8, 128), jnp.float32),
                jax.ShapeDtypeStruct((16, 2, ROWS, WIDTH), jnp.bfloat16),
            ),
            in_specs=[smem, smem, hbm, hbm],
            out_specs=(hbm, hbm, vmem, hbm),
            scratch_shapes=[
                emb,
                emb,
                acc,
                acc,
                pltpu.VMEM((2 + len(STEPS) - DIRECT, 2, 2 * PIECE, WIDTH), jnp.bfloat16),
                pltpu.VMEM((4, 8, 2 * PIECE), jnp.float32),
                pltpu.SemaphoreType.DMA((2, QUARTERS)),
                pltpu.SemaphoreType.DMA((2, 2, 2)),
                pltpu.SemaphoreType.DMA((2,)),
                pltpu.SemaphoreType.DMA((N_SENDS,)),
                pltpu.SemaphoreType.DMA((16, 2, QUARTERS, 3)),
                pltpu.VMEM((16, 4, 8, 128), jnp.float32),
                pltpu.SemaphoreType.DMA((16,)),
                pltpu.SemaphoreType.DMA((16,)),
            ],
            compiler_params=pltpu.CompilerParams(
                collective_id=0, has_side_effects=True, vmem_limit_bytes=62 * 2**20
            ),
        )(log_temp.reshape(1), logit_bias.reshape(1), img_emb, txt_emb)
        gx, gy, loss, gtemp, gbias = pl.pallas_call(
            project_kernel,
            grid=(ROWS // 512,),
            out_shape=(acc_shape, acc_shape, one, one, one),
            in_specs=[pl.BlockSpec((5, 8, 128), lambda i: (0, 0, 0)), block, block, block, block],
            out_specs=(block, block, smem, smem, smem),
        )(stats, img_emb, txt_emb, au, av)
        return loss[0], gx, gy, gtemp[0], gbias[0]

    return jax.shard_map(
        local_fn,
        mesh=mesh,
        in_specs=(P("dp", None), P("dp", None), P(), P()),
        out_specs=(P(), P("dp", None), P("dp", None), P(), P()),
        check_vma=False,
    )
```
